8 devices in a mesh: rep: 1 (over z), ep: 2 (over y), fsdp: 4 (over x, core).
Axes of the slice: x: 2, y: 2, z: 1, core: 2. Of those that a mesh axis runs over, the one named last changes fastest.
Arguments:
- x_in: bfloat16 [16384, 2048], P(('rep', 'ep', 'fsdp'))
- norm_w: float32 [2, 2048], replicated
- router_w: bfloat16 [2, 2048, 4], replicated
- gate_w: bfloat16 [2, 4, 2048, 5632], P(None, 'ep', None, 'fsdp')
- up_w: bfloat16 [2, 4, 2048, 5632], P(None, 'ep', None, 'fsdp')
- down_w: bfloat16 [2, 4, 5632, 2048], P(None, 'ep', 'fsdp')
- routes: int32 [2, 16384, 2], P(None, ('rep', 'ep', 'fsdp'))
Outputs:
- output: bfloat16 [16384, 2048], P(('rep', 'ep', 'fsdp'))
All inputs are finite; a program needn't handle non-finite values.
Results may differ from the reference program's by a relative error of at most 0.0124657.
Values are sent between devices in bfloat16 or wider.
A program may use at most 1 GiB of HBM per device.

```python
import jax
import jax.numpy as jnp
from jax import lax
import numpy as np

EXPERTS = 4
TOP = 2
D_MODEL = 2048
FF_DIM = 5632
TOK_DEV = 2048
DEV_PART = 8
LAYERS = 2

NORM_EPS = 1e-5
CAPACITY = 8 * ((2 * TOK_DEV * TOP + 8 * EXPERTS - 1) // (8 * EXPERTS))
TOKENS = TOK_DEV * DEV_PART
ROW_CAP = DEV_PART * CAPACITY


def count_pattern(n_pairs, n_experts, capacity):
    counts = [1 + ((capacity - 1) * (n_experts - 1 - position)) // (n_experts - 1) for position in range(n_experts)]
    cursor = 1
    while sum(counts) < n_pairs:
        if counts[cursor] < capacity:
            counts[cursor] += 1
        cursor = cursor % (n_experts - 1) + 1
    while sum(counts) > n_pairs:
        if counts[cursor] > 1:
            counts[cursor] -= 1
        cursor = cursor % (n_experts - 1) + 1
    return counts


def draw_routes(route_key):
    counts = count_pattern(TOK_DEV * TOP, EXPERTS, CAPACITY)
    pattern = np.repeat(np.arange(EXPERTS), counts).astype(np.int32)

    def one_block(block_key):
        key_label, key_order = jax.random.split(block_key)
        relabel = jax.random.permutation(key_label, EXPERTS)
        expert_ids = relabel[pattern].reshape(TOP, TOK_DEV).T
        token_order = jax.random.permutation(key_order, TOK_DEV)
        return expert_ids[token_order]

    block_keys = jax.random.split(route_key, LAYERS * DEV_PART)
    all_blocks = jax.vmap(one_block)(block_keys)
    return all_blocks.reshape(LAYERS, TOKENS, TOP).astype(jnp.int32)


def setup_inputs(seed: int = 0, part: int = 0) -> dict:
    weight_keys = jax.random.split(jax.random.key(seed), 5)
    part_keys = jax.random.split(jax.random.fold_in(jax.random.key(seed + 1), part), 2)
    x_in = jax.random.normal(part_keys[0], (TOKENS, D_MODEL), jnp.float32).astype(jnp.bfloat16)
    norm_w = 1.0 + 0.25 * jax.random.normal(weight_keys[0], (LAYERS, D_MODEL), jnp.float32)
    router_w = (jax.random.normal(weight_keys[1], (LAYERS, D_MODEL, EXPERTS), jnp.float32) * D_MODEL ** -0.5).astype(jnp.bfloat16)
    gate_w = (jax.random.normal(weight_keys[2], (LAYERS, EXPERTS, D_MODEL, FF_DIM), jnp.float32) * D_MODEL ** -0.5).astype(jnp.bfloat16)
    up_w = (jax.random.normal(weight_keys[3], (LAYERS, EXPERTS, D_MODEL, FF_DIM), jnp.float32) * D_MODEL ** -0.5).astype(jnp.bfloat16)
    down_w = (jax.random.normal(weight_keys[4], (LAYERS, EXPERTS, FF_DIM, D_MODEL), jnp.float32) * (1.5 * (TOP / FF_DIM) ** 0.5)).astype(jnp.bfloat16)
    routes = draw_routes(part_keys[1])
    return {"x_in": x_in, "norm_w": norm_w, "router_w": router_w, "gate_w": gate_w, "up_w": up_w, "down_w": down_w, "routes": routes}


def rms_norm(stream, norm_row):
    widened = stream.astype(jnp.float32)
    inv_rms = lax.rsqrt(jnp.mean(widened * widened, axis=-1, keepdims=True) + NORM_EPS)
    return (widened * inv_rms * norm_row).astype(jnp.bfloat16)


def moe_layer(stream, layer_params):
    norm_row, router_l, gate_l, up_l, down_l, routes_l = layer_params
    hidden = rms_norm(stream, norm_row)
    logits = jnp.dot(hidden, router_l, preferred_element_type=jnp.float32)
    gate_probs = jax.nn.softmax(jnp.take_along_axis(logits, routes_l, axis=1), axis=-1)

    def expert_step(mixed_sum, expert_params):
        expert_id, gate_e, up_e, down_e = expert_params
        is_chosen = routes_l == expert_id
        token_gate = jnp.sum(jnp.where(is_chosen, gate_probs, 0.0), axis=1)
        token_rows = jnp.nonzero(jnp.any(is_chosen, axis=1), size=ROW_CAP, fill_value=0)[0]
        row_valid = jnp.arange(ROW_CAP) < jnp.sum(is_chosen)
        row_gate = jnp.where(row_valid, token_gate[token_rows], 0.0)
        picked = hidden[token_rows]
        pre_gate = jnp.dot(picked, gate_e, preferred_element_type=jnp.float32)
        pre_up = jnp.dot(picked, up_e, preferred_element_type=jnp.float32)
        inner_act = (jax.nn.silu(pre_gate) * pre_up).astype(jnp.bfloat16)
        expert_out = jnp.dot(inner_act, down_e, preferred_element_type=jnp.float32).astype(jnp.bfloat16)
        mixed_sum = mixed_sum.at[token_rows].add(row_gate[:, None] * expert_out.astype(jnp.float32))
        return mixed_sum, None

    start_sum = jnp.zeros(stream.shape, jnp.float32)
    mixed_sum, _ = lax.scan(expert_step, start_sum, (jnp.arange(EXPERTS), gate_l, up_l, down_l))
    return (stream.astype(jnp.float32) + mixed_sum).astype(jnp.bfloat16), None


def reference(x_in, norm_w, router_w, gate_w, up_w, down_w, routes):
    final_stream, _ = lax.scan(moe_layer, x_in, (norm_w, router_w, gate_w, up_w, down_w, routes))
    return final_stream
```

```python
import jax
import jax.numpy as jnp
from jax import lax
from jax.experimental import pallas as pl
from jax.experimental.pallas import tpu as pltpu
from jax.sharding import PartitionSpec as P


NORM_EPS = 1e-5
ROW_TILE = 256
COL_CHUNK = 256
OUT_TILE = 1024
MIX_TILE = 256


def rms_norm(stream, norm_row):
    widened = stream.astype(jnp.float32)
    inv_rms = lax.rsqrt(jnp.mean(widened * widened, axis=-1, keepdims=True) + NORM_EPS)
    return (widened * inv_rms * norm_row).astype(jnp.bfloat16)


def block_order(routes_l, experts):
    tok_dev = routes_l.shape[0]
    ids = jnp.arange(experts, dtype=jnp.int32)
    chosen = (routes_l[:, 0:1] == ids) | (routes_l[:, 1:2] == ids)
    counts = jnp.sum(chosen.astype(jnp.int32), axis=0)
    common = jnp.sum(jnp.where(counts == tok_dev, ids, 0))
    second = routes_l[:, 0] + routes_l[:, 1] - common
    key = second * tok_dev + jnp.arange(tok_dev, dtype=jnp.int32)
    place = jnp.sum((key[:, None] < key[None, :]).astype(jnp.int32), axis=0)
    start = jnp.sum((second[:, None] < ids).astype(jnp.int32), axis=0)
    stop = jnp.sum((second[:, None] <= ids).astype(jnp.int32), axis=0)
    start = jnp.where(ids == common, 0, start)
    stop = jnp.where(ids == common, tok_dev, stop)
    return place, start, stop


def at_place(place, values):
    slots = jnp.arange(place.shape[0], dtype=jnp.int32)
    return jnp.sum(jnp.where(place[:, None] == slots[None, :], values[:, None], 0), axis=0)


def tile_of(step, span):
    return jnp.minimum(span[0] + step, span[1])


def inner_rows(after, span, rows, gates, ups):
    tok, d_model = rows.shape
    part = gates[0][0].shape[-1]
    n_parts = len(gates)
    width = n_parts * part
    sources = list(gates) + list(ups)

    def kernel(span, after_ref, rows_ref, *refs):
        weight_refs, (act_ref, held, sems) = refs[:len(sources)], refs[len(sources):]
        i = pl.program_id(0)

        def copies(q):
            found = []
            for m in range(2):
                ref, lead = weight_refs[m * n_parts + q], sources[m * n_parts + q][1]
                found.append(pltpu.make_async_copy(ref.at[lead] if lead else ref, held.at[m, :, pl.ds(q * part, part)], sems.at[m, q]))
            return found

        @pl.when(i == 0)
        def _():
            for q in range(n_parts):
                for copy in copies(q):
                    copy.start()

        @pl.when(span[0] + i <= span[1])
        def _():
            rows = rows_ref[...]
            ready = 0
            for first in range(0, width, COL_CHUNK):
                cols = slice(first, first + COL_CHUNK)
                while ready * part < first + COL_CHUNK and ready < n_parts:
                    @pl.when(i == 0)
                    def _():
                        for copy in copies(ready):
                            copy.wait()

                    ready += 1
                pre_gate = jnp.dot(rows, held[0, :, cols], preferred_element_type=jnp.float32)
                pre_up = jnp.dot(rows, held[1, :, cols], preferred_element_type=jnp.float32)
                act_ref[:, cols] = (jax.nn.silu(pre_gate) * pre_up).astype(jnp.bfloat16)

    return pl.pallas_call(
        kernel,
        out_shape=jax.ShapeDtypeStruct((tok, width), jnp.bfloat16),
        grid_spec=pltpu.PrefetchScalarGridSpec(
            num_scalar_prefetch=1, grid=(tok // ROW_TILE,),
            in_specs=[pl.BlockSpec(memory_space=pl.ANY), pl.BlockSpec((ROW_TILE, d_model), lambda i, s: (tile_of(i, s), 0))]
            + [pl.BlockSpec(memory_space=pl.ANY)] * len(sources),
            out_specs=pl.BlockSpec((ROW_TILE, width), lambda i, s: (tile_of(i, s), 0)),
            scratch_shapes=[pltpu.VMEM((2, d_model, width), jnp.bfloat16), pltpu.SemaphoreType.DMA((2, n_parts))]),
        compiler_params=pltpu.CompilerParams(dimension_semantics=("arbitrary",)),
        cost_estimate=pl.CostEstimate(flops=2 * tok * d_model * width, bytes_accessed=4 * d_model * width, transcendentals=0),
        name="inner_rows",
    )(span, after, rows, *[s[0] for s in sources])


def outer_rows(after, span, acts, downs):
    tok = acts[0].shape[0]
    part = acts[0].shape[1] * len(acts) // len(downs)
    cols = sum(piece[3] for piece in downs[0])
    tile = min(OUT_TILE, cols)
    flat, moves = [], [[] for _ in range(cols // tile)]
    for q, pieces in enumerate(downs):
        at = 0
        for array, lead, first, count in pieces:
            done = 0
            while done < count:
                size = min(count - done, tile - at % tile)
                moves[at // tile].append((len(flat), lead, first + done, q * part, at % tile, size))
                at, done = at + size, done + size
            flat.append(array)
    most = max(len(m) for m in moves)

    def kernel(span, after_ref, *refs):
        act_refs, down_refs = refs[:len(acts)], refs[len(acts):len(acts) + len(flat)]
        out_ref, held, sems = refs[len(acts) + len(flat):]
        c, i = pl.program_id(0), pl.program_id(1)

        def copies(n):
            return [pltpu.make_async_copy(down_refs[a].at[lead + (slice(None), pl.ds(first, size))],
                                          held.at[n, pl.ds(row, part), pl.ds(col, size)], sems.at[n, j])
                    for j, (a, lead, first, row, col, size) in enumerate(moves[n])]

        @pl.when((c == 0) & (i == 0))
        def _():
            for n in range(len(moves)):
                for copy in copies(n):
                    copy.start()

        for n in range(len(moves)):
            @pl.when((c == n) & (i == 0))
            def _():
                for copy in copies(n):
                    copy.wait()

        @pl.when(span[0] + i <= span[1])
        def _():
            total, at = None, 0
            for act in act_refs:
                depth = act.shape[1]
                term = jnp.dot(act[...], held[c, at:at + depth], preferred_element_type=jnp.float32)
                total = term if total is None else total + term
                at += depth
            out_ref[...] = total.astype(jnp.bfloat16)

    return pl.pallas_call(
        kernel,
        out_shape=jax.ShapeDtypeStruct((tok, cols), jnp.bfloat16),
        grid_spec=pltpu.PrefetchScalarGridSpec(
            num_scalar_prefetch=1, grid=(cols // tile, tok // ROW_TILE),
            in_specs=[pl.BlockSpec(memory_space=pl.ANY)]
            + [pl.BlockSpec((ROW_TILE, a.shape[1]), lambda c, i, s: (tile_of(i, s), 0)) for a in acts]
            + [pl.BlockSpec(memory_space=pl.ANY)] * len(flat),
            out_specs=pl.BlockSpec((ROW_TILE, tile), lambda c, i, s: (tile_of(i, s), c)),
            scratch_shapes=[pltpu.VMEM((len(moves), part * len(downs), tile), jnp.bfloat16),
                            pltpu.SemaphoreType.DMA((len(moves), most))]),
        compiler_params=pltpu.CompilerParams(dimension_semantics=("arbitrary", "arbitrary")),
        cost_estimate=pl.CostEstimate(flops=tok * cols * part * len(downs), bytes_accessed=2 * len(downs) * cols * part,
                                      transcendentals=0),
        name="outer_rows",
    )(span, after, *acts, *flat)


def mix(ranges, stream, gates, parts):
    tok, d_model = stream.shape
    cuts = max(len(p) for p in parts)
    width = d_model // cuts

    def kernel(ranges, stream_ref, gates_ref, *refs):
        out_ref = refs[-1]
        row = lax.broadcasted_iota(jnp.int32, (MIX_TILE, 1), 0) + pl.program_id(0) * MIX_TILE
        for c in range(cuts):
            cols = slice(c * width, (c + 1) * width)
            mixed = jnp.zeros((MIX_TILE, width), jnp.float32)
            at = 0
            for e, pieces in enumerate(parts):
                ref = refs[at + c][...] if len(pieces) > 1 else refs[at][:, cols]
                at += len(pieces)
                picked = (row >= ranges[e]) & (row < ranges[len(parts) + e])
                mixed += jnp.where(picked, gates_ref[:, e:e + 1] * ref.astype(jnp.float32), 0.0)
            out_ref[:, cols] = (stream_ref[:, cols].astype(jnp.float32) + mixed).astype(jnp.bfloat16)

    flat = [p for pieces in parts for p in pieces]
    row_spec = lambda cols: pl.BlockSpec((MIX_TILE, cols), lambda i, s: (i, 0))
    return pl.pallas_call(
        kernel,
        out_shape=jax.ShapeDtypeStruct((tok, d_model), jnp.bfloat16),
        grid_spec=pltpu.PrefetchScalarGridSpec(
            num_scalar_prefetch=1, grid=(tok // MIX_TILE,),
            in_specs=[row_spec(d_model), row_spec(gates.shape[1])] + [row_spec(p.shape[1]) for p in flat],
            out_specs=row_spec(d_model)),
        compiler_params=pltpu.CompilerParams(dimension_semantics=("arbitrary",)),
        cost_estimate=pl.CostEstimate(flops=20 * tok * d_model, bytes_accessed=12 * tok * d_model, transcendentals=0),
        name="mix",
    )(ranges, stream, gates, *flat)


CUTS = ((1, 4), (1, 4))


def solution(mesh):
    owners, shards = mesh.shape["ep"], mesh.shape["fsdp"]
    token_spec = P(("rep", "ep", "fsdp"), None)
    expert_in_spec = P(None, "ep", None, "fsdp")
    expert_out_spec = P(None, "ep", "fsdp", None)
    route_spec = P(None, ("rep", "ep", "fsdp"), None)
    swap = [(i, owners - 1 - i) for i in range(owners)]

    def device_step(x_in, norm_w, router_w, gate_w, up_w, down_w, routes):
        layers, tok_dev, _ = routes.shape
        experts = router_w.shape[2]
        n_local = gate_w.shape[1]
        d_model = x_in.shape[1]
        mine = lax.axis_index("ep")

        def across(v):
            return lax.ppermute(v, "fsdp", [(i, (i + shards // 2) % shards) for i in range(shards)])

        def beside(v):
            return lax.ppermute(v, "fsdp", [(i, i ^ 1) for i in range(shards)])

        near = []
        for param in (gate_w, up_w, down_w):
            near.append(beside(param))
        far = [[None] * n_local for _ in range(layers)]
        for layer in range(layers):
            for k in range(n_local):
                cuts = CUTS[layer][k]
                width = d_model // cuts
                pieces = [gate_w[layer, k], up_w[layer, k]]
                pieces += [down_w[layer, k][:, c * width:(c + 1) * width] for c in range(cuts)]
                out = []
                for piece in pieces:
                    there = across(piece)
                    out.append((there, beside(there)))
                far[layer][k] = out

        orders = [block_order(routes[layer], experts) for layer in range(layers)]
        bounds = jnp.stack([jnp.stack(o[1:]) for o in orders])
        peer_bounds = lax.ppermute(bounds, "ep", swap)
        tokens = jnp.arange(tok_dev, dtype=jnp.int32)

        def spans(table, layer):
            start, stop = table[layer, 0], table[layer, 1]
            both = jnp.stack([start // ROW_TILE, (stop - 1) // ROW_TILE], axis=1)
            return [jnp.where(mine == 0, both[k], both[n_local + k]) for k in range(n_local)]

        def own_first(table):
            return jnp.where(mine == 0, table, jnp.roll(table, n_local, axis=-1))

        stream = x_in
        for layer in range(layers):
            place = orders[layer][0]
            if layer == 0:
                index = at_place(place, tokens)
            else:
                index = at_place(place, orders[layer - 1][0])
            stream = stream[index]
            hidden = rms_norm(stream, norm_w[layer])
            peer_hidden = lax.ppermute(hidden, "ep", swap)
            logits = own_first(jnp.dot(hidden, router_w[layer], preferred_element_type=jnp.float32))
            ranges = own_first(bounds[layer])
            row = tokens[:, None]
            picked = (row >= ranges[0]) & (row < ranges[1])
            top = jnp.max(jnp.where(picked, logits, -jnp.inf), axis=-1, keepdims=True)
            weight = jnp.where(picked, jnp.exp(jnp.where(picked, logits - top, 0.0)), 0.0)
            gates = weight / jnp.sum(weight, axis=-1, keepdims=True)

            own_spans, peer_spans = spans(bounds, layer), spans(peer_bounds, layer)

            def close(after, k, span, rows):
                return inner_rows(after, span, rows, [(gate_w, (layer, k)), (near[0], (layer, k))],
                                  [(up_w, (layer, k)), (near[1], (layer, k))])

            def distant(after, k, span, rows):
                pair = far[layer][k]
                return inner_rows(after, span, rows, [(v, ()) for v in pair[0]], [(v, ()) for v in pair[1]])

            def outer(after, k, span, acts, pieces):
                cols = far[layer][k][2][0].shape[1]
                first, count = pieces[0] * cols, len(pieces) * cols
                return outer_rows(after, span, acts, [[(down_w, (layer, k), first, count)], [(near[2], (layer, k), first, count)]]
                                  + [[(far[layer][k][2 + c][side], (), 0, cols) for c in pieces] for side in range(2)])

            def step(make, *args):
                made = make(*args)
                return made

            def send_back(made):
                return lax.ppermute(made, "ep", swap)

            own_close, peer_close = [hidden], [None]
            for k in range(n_local):
                own_close.append(step(close, own_close[-1], k, own_spans[k], hidden))
            own_far = step(distant, own_close[-1], 0, own_spans[0], hidden)
            peer_close[0] = own_far
            for k in range(n_local):
                peer_close.append(step(close, peer_close[-1], k, peer_spans[k], peer_hidden))
            own_parts, back_parts, last = [], [], peer_close[-1]
            for k in range(n_local):
                every = list(range(CUTS[layer][k]))
                last = peer_far = step(distant, last, k, peer_spans[k], peer_hidden)
                back = []
                for c in every:
                    last = step(outer, last, k, peer_spans[k], [peer_close[1 + k], peer_far], [c])
                    back.append(send_back(last))
                if k > 0:
                    last = own_far = step(distant, last, k, own_spans[k], hidden)
                last = step(outer, last, k, own_spans[k], [own_close[1 + k], own_far], every)
                own_parts.append([last])
                back_parts.append(back)
            stream = mix(ranges.reshape(-1), stream, gates, own_parts + back_parts)
        return stream[orders[layers - 1][0]]

    return jax.shard_map(device_step, mesh=mesh,
                         in_specs=(token_spec, P(), P(), expert_in_spec, expert_in_spec, expert_out_spec, route_spec),
                         out_specs=token_spec, check_vma=False)
```

```python
import jax
import jax.numpy as jnp
from jax import lax
from jax.experimental import pallas as pl
from jax.experimental.pallas import tpu as pltpu
from jax.sharding import PartitionSpec as P


NORM_EPS = 1e-5
ROW_TILE = 256
COL_CHUNK = 256
OUT_TILE = 1024
MIX_TILE = 256


def rms_norm(stream, norm_row):
    widened = stream.astype(jnp.float32)
    inv_rms = lax.rsqrt(jnp.mean(widened * widened, axis=-1, keepdims=True) + NORM_EPS)
    return (widened * inv_rms * norm_row).astype(jnp.bfloat16)


def block_order(routes_l, experts):
    tok_dev = routes_l.shape[0]
    ids = jnp.arange(experts, dtype=jnp.int32)
    chosen = (routes_l[:, 0:1] == ids) | (routes_l[:, 1:2] == ids)
    counts = jnp.sum(chosen.astype(jnp.int32), axis=0)
    common = jnp.sum(jnp.where(counts == tok_dev, ids, 0))
    second = routes_l[:, 0] + routes_l[:, 1] - common
    key = second * tok_dev + jnp.arange(tok_dev, dtype=jnp.int32)
    place = jnp.sum((key[:, None] < key[None, :]).astype(jnp.int32), axis=0)
    start = jnp.sum((second[:, None] < ids).astype(jnp.int32), axis=0)
    stop = jnp.sum((second[:, None] <= ids).astype(jnp.int32), axis=0)
    start = jnp.where(ids == common, 0, start)
    stop = jnp.where(ids == common, tok_dev, stop)
    return place, start, stop


def at_place(place, values):
    slots = jnp.arange(place.shape[0], dtype=jnp.int32)
    return jnp.sum(jnp.where(place[:, None] == slots[None, :], values[:, None], 0), axis=0)


def tile_of(step, span):
    return jnp.minimum(span[0] + step, span[1])


def inner_rows(after, span, rows, gates, ups):
    tok, d_model = rows.shape
    part = gates[0][0].shape[-1]
    n_parts = len(gates)
    width = n_parts * part
    sources = list(gates) + list(ups)
    chunks = []
    for first in range(0, width, COL_CHUNK):
        cuts = sorted({first, first + COL_CHUNK} | {q * part for q in range(n_parts) if first < q * part < first + COL_CHUNK})
        chunks.append([(lo // part, lo % part, hi - lo) for lo, hi in zip(cuts, cuts[1:])])

    def kernel(span, after_ref, rows_ref, *refs):
        weight_refs, (act_ref, held, sems) = refs[:len(sources)], refs[len(sources):]
        i = pl.program_id(0)

        def copies(chunk):
            found = []
            for m in range(2):
                for q, first, size in chunks[chunk]:
                    ref, lead = weight_refs[m * n_parts + q], sources[m * n_parts + q][1]
                    at = q * part + first
                    found.append(pltpu.make_async_copy(ref.at[lead + (slice(None), pl.ds(first, size))],
                                                       held.at[m, :, pl.ds(at, size)], sems.at[chunk, len(found)]))
            return found

        @pl.when(i == 0)
        def _():
            for chunk in range(len(chunks)):
                for copy in copies(chunk):
                    copy.start()

        def columns(chunk):
            cols = slice(chunk * COL_CHUNK, (chunk + 1) * COL_CHUNK)
            pre_gate = jnp.dot(rows_ref[...], held[0, :, cols], preferred_element_type=jnp.float32)
            pre_up = jnp.dot(rows_ref[...], held[1, :, cols], preferred_element_type=jnp.float32)
            act_ref[:, cols] = (jax.nn.silu(pre_gate) * pre_up).astype(jnp.bfloat16)

        @pl.when(i == 0)
        def _():
            for chunk in range(len(chunks)):
                for copy in copies(chunk):
                    copy.wait()
                columns(chunk)

        @pl.when((i > 0) & (span[0] + i <= span[1]))
        def _():
            for chunk in range(len(chunks)):
                columns(chunk)

    return pl.pallas_call(
        kernel,
        out_shape=jax.ShapeDtypeStruct((tok, width), jnp.bfloat16),
        grid_spec=pltpu.PrefetchScalarGridSpec(
            num_scalar_prefetch=1, grid=(tok // ROW_TILE,),
            in_specs=[pl.BlockSpec(memory_space=pl.ANY), pl.BlockSpec((ROW_TILE, d_model), lambda i, s: (tile_of(i, s), 0))]
            + [pl.BlockSpec(memory_space=pl.ANY)] * len(sources),
            out_specs=pl.BlockSpec((ROW_TILE, width), lambda i, s: (tile_of(i, s), 0)),
            scratch_shapes=[pltpu.VMEM((2, d_model, width), jnp.bfloat16), pltpu.SemaphoreType.DMA((len(chunks), 2 * n_parts))]),
        compiler_params=pltpu.CompilerParams(dimension_semantics=("arbitrary",)),
        cost_estimate=pl.CostEstimate(flops=2 * tok * d_model * width, bytes_accessed=4 * d_model * width, transcendentals=0),
        name="inner_rows",
    )(span, after, rows, *[s[0] for s in sources])


def outer_rows(after, span, acts, downs):
    tok = acts[0].shape[0]
    depth_all = sum(a.shape[1] for a in acts)
    cols = sum(piece[3] for piece in downs[0][2])
    tile = min(OUT_TILE, cols)
    flat, moves, held_row = [], [[] for _ in range(cols // tile)], 0
    for first_row, rows, pieces in downs:
        at = 0
        for array, lead, first, count in pieces:
            done = 0
            while done < count:
                size = min(count - done, tile - at % tile)
                moves[at // tile].append((len(flat), lead, first_row, rows, first + done, held_row, at % tile, size))
                at, done = at + size, done + size
            flat.append(array)
        held_row += rows
    most = max(len(m) for m in moves)

    def kernel(span, after_ref, *refs):
        act_refs, down_refs = refs[:len(acts)], refs[len(acts):len(acts) + len(flat)]
        out_ref, held, sems = refs[len(acts) + len(flat):]
        c, i = pl.program_id(0), pl.program_id(1)

        def copies(n):
            return [pltpu.make_async_copy(down_refs[a].at[lead + (pl.ds(first_row, rows), pl.ds(first, size))],
                                          held.at[n, pl.ds(row, rows), pl.ds(col, size)], sems.at[n, j])
                    for j, (a, lead, first_row, rows, first, row, col, size) in enumerate(moves[n])]

        @pl.when((c == 0) & (i == 0))
        def _():
            for n in range(len(moves)):
                for copy in copies(n):
                    copy.start()

        for n in range(len(moves)):
            @pl.when((c == n) & (i == 0))
            def _():
                for copy in copies(n):
                    copy.wait()

        @pl.when(span[0] + i <= span[1])
        def _():
            total, at = None, 0
            for act in act_refs:
                depth = act.shape[1]
                term = jnp.dot(act[...], held[c, at:at + depth], preferred_element_type=jnp.float32)
                total = term if total is None else total + term
                at += depth
            out_ref[...] = total.astype(jnp.bfloat16)

    return pl.pallas_call(
        kernel,
        out_shape=jax.ShapeDtypeStruct((tok, cols), jnp.bfloat16),
        grid_spec=pltpu.PrefetchScalarGridSpec(
            num_scalar_prefetch=1, grid=(cols // tile, tok // ROW_TILE),
            in_specs=[pl.BlockSpec(memory_space=pl.ANY)]
            + [pl.BlockSpec((ROW_TILE, a.shape[1]), lambda c, i, s: (tile_of(i, s), 0)) for a in acts]
            + [pl.BlockSpec(memory_space=pl.ANY)] * len(flat),
            out_specs=pl.BlockSpec((ROW_TILE, tile), lambda c, i, s: (tile_of(i, s), c)),
            scratch_shapes=[pltpu.VMEM((len(moves), depth_all, tile), jnp.bfloat16),
                            pltpu.SemaphoreType.DMA((len(moves), most))]),
        compiler_params=pltpu.CompilerParams(dimension_semantics=("arbitrary", "arbitrary")),
        cost_estimate=pl.CostEstimate(flops=tok * cols * depth_all, bytes_accessed=2 * depth_all * cols,
                                      transcendentals=0),
        name="outer_rows",
    )(span, after, *acts, *flat)


def mix(ranges, stream, gates, parts, norm_row=None):
    tok, d_model = stream.shape
    count = len(parts)
    flat = [p for pieces in parts for p in pieces]
    extra = [] if norm_row is None else [norm_row.reshape(1, d_model)]

    def kernel(ranges, stream_ref, gates_ref, *refs):
        outs, total = refs[len(flat) + len(extra):-1], refs[-1]
        first = pl.program_id(0) * MIX_TILE
        row = lax.broadcasted_iota(jnp.int32, (MIX_TILE, 1), 0) + first
        total[...] = stream_ref[...].astype(jnp.float32)
        at = 0
        for e, pieces in enumerate(parts):
            here = refs[at:at + len(pieces)]
            at += len(pieces)

            @pl.when((ranges[e] < first + MIX_TILE) & (ranges[count + e] > first))
            def _():
                picked = (row >= ranges[e]) & (row < ranges[count + e])
                for c, ref in enumerate(here):
                    cols = slice(c * ref.shape[1], (c + 1) * ref.shape[1])
                    total[:, cols] += jnp.where(picked, gates_ref[:, e:e + 1] * ref[...].astype(jnp.float32), 0.0)
        rounded = total[...].astype(jnp.bfloat16)
        outs[0][...] = rounded
        if extra:
            widened = rounded.astype(jnp.float32)
            inv_rms = lax.rsqrt(jnp.sum(widened * widened, axis=-1, keepdims=True) / d_model + NORM_EPS)
            outs[1][...] = (widened * inv_rms * refs[len(flat)][...]).astype(jnp.bfloat16)

    def part_spec(e, cols):
        def tile(i, ranges):
            return jnp.clip(i, ranges[e] // MIX_TILE, (ranges[count + e] - 1) // MIX_TILE), 0

        return pl.BlockSpec((MIX_TILE, cols), tile)

    row_spec = lambda cols: pl.BlockSpec((MIX_TILE, cols), lambda i, s: (i, 0))
    return pl.pallas_call(
        kernel,
        out_shape=[jax.ShapeDtypeStruct((tok, d_model), jnp.bfloat16)] * (1 + len(extra)),
        grid_spec=pltpu.PrefetchScalarGridSpec(
            num_scalar_prefetch=1, grid=(tok // MIX_TILE,),
            in_specs=[row_spec(d_model), row_spec(gates.shape[1])] + [part_spec(e, p.shape[1]) for e, pieces in enumerate(parts) for p in pieces]
            + [pl.BlockSpec((1, d_model), lambda i, s: (0, 0))] * len(extra),
            out_specs=[row_spec(d_model)] * (1 + len(extra)),
            scratch_shapes=[pltpu.VMEM((MIX_TILE, d_model), jnp.float32)]),
        compiler_params=pltpu.CompilerParams(dimension_semantics=("arbitrary",)),
        cost_estimate=pl.CostEstimate(flops=20 * tok * d_model, bytes_accessed=12 * tok * d_model, transcendentals=0),
        name="mix",
    )(ranges, stream, gates, *flat, *extra)


CUTS = (1, 4)
FF_CUTS = (((0, 1408),), ((0, 768), (768, 1408)))


def solution(mesh):
    owners, shards = mesh.shape["ep"], mesh.shape["fsdp"]
    token_spec = P(("rep", "ep", "fsdp"), None)
    expert_in_spec = P(None, "ep", None, "fsdp")
    expert_out_spec = P(None, "ep", "fsdp", None)
    route_spec = P(None, ("rep", "ep", "fsdp"), None)
    swap = [(i, owners - 1 - i) for i in range(owners)]

    def device_step(x_in, norm_w, router_w, gate_w, up_w, down_w, routes):
        layers, tok_dev, _ = routes.shape
        experts = router_w.shape[2]
        n_local = gate_w.shape[1]
        d_model = x_in.shape[1]
        mine = lax.axis_index("ep")

        def across(v):
            return lax.ppermute(v, "fsdp", [(i, (i + shards // 2) % shards) for i in range(shards)])

        def beside(v):
            return lax.ppermute(v, "fsdp", [(i, i ^ 1) for i in range(shards)])

        near = []
        for param in (gate_w, up_w, down_w):
            near.append(beside(param))
        far = [[None] * n_local for _ in range(layers)]
        serial = 0
        for layer in range(layers):
            for k in range(n_local):
                width = d_model // CUTS[k]
                first_gate = lax.optimization_barrier(gate_w) if serial == 0 else gate_w
                pieces = [w[layer, k][:, lo:hi] for lo, hi in FF_CUTS[k] for w in (first_gate, up_w)]
                pieces += [down_w[layer, k][:, c * width:(c + 1) * width] for c in range(CUTS[k])]
                out = []
                for piece in pieces:
                    there = across(piece)
                    out.append((there, beside(there)))
                    serial += 1
                inner = 2 * len(FF_CUTS[k])
                far[layer][k] = (out[0:inner:2], out[1:inner:2], out[inner:])

        orders = [block_order(routes[layer], experts) for layer in range(layers)]
        bounds = jnp.stack([jnp.stack(o[1:]) for o in orders])
        peer_bounds = lax.ppermute(bounds, "ep", swap)
        tokens = jnp.arange(tok_dev, dtype=jnp.int32)

        def spans(table, layer):
            start, stop = table[layer, 0], table[layer, 1]
            both = jnp.stack([start // ROW_TILE, (stop - 1) // ROW_TILE], axis=1)
            return [jnp.where(mine == 0, both[k], both[n_local + k]) for k in range(n_local)]

        def own_first(table):
            return jnp.where(mine == 0, table, jnp.roll(table, n_local, axis=-1))

        stream, hidden = x_in, None
        for layer in range(layers):
            place = orders[layer][0]
            if layer == 0:
                index = at_place(place, tokens)
                stream = stream[index]
                hidden = rms_norm(stream, norm_w[layer])
            else:
                index = at_place(place, orders[layer - 1][0])
                hidden = hidden[index]
            peer_hidden = lax.ppermute(hidden, "ep", swap)
            logits = own_first(jnp.dot(hidden, router_w[layer], preferred_element_type=jnp.float32))
            ranges = own_first(bounds[layer])
            row = tokens[:, None]
            picked = (row >= ranges[0]) & (row < ranges[1])
            top = jnp.max(jnp.where(picked, logits, -jnp.inf), axis=-1, keepdims=True)
            weight = jnp.where(picked, jnp.exp(jnp.where(picked, logits - top, 0.0)), 0.0)
            gates = weight / jnp.sum(weight, axis=-1, keepdims=True)

            own_spans, peer_spans = spans(bounds, layer), spans(peer_bounds, layer)

            def close(after, k, span, rows):
                return inner_rows(after, span, rows, [(gate_w, (layer, k)), (near[0], (layer, k))],
                                  [(up_w, (layer, k)), (near[1], (layer, k))])

            def distant(after, k, span, rows, j):
                gates_far, ups_far, _ = far[layer][k]
                return inner_rows(after, span, rows, [(v, ()) for v in gates_far[j]], [(v, ()) for v in ups_far[j]])

            def outer(after, k, span, acts, pieces):
                down_far = far[layer][k][2]
                ff, cols = down_far[0][0].shape
                first, count = pieces[0] * cols, len(pieces) * cols
                downs = [(0, ff, [(down_w, (layer, k), first, count)]), (0, ff, [(near[2], (layer, k), first, count)])]
                downs += [(lo, hi - lo, [(down_far[c][side], (), 0, cols) for c in pieces]) for lo, hi in FF_CUTS[k] for side in range(2)]
                return outer_rows(after, span, acts, downs)

            def step(make, *args):
                made = make(*args)
                return made

            def send_back(made):
                return lax.ppermute(made, "ep", swap)

            own_close = [hidden]
            for k in range(n_local):
                own_close.append(step(close, own_close[-1], k, own_spans[k], hidden))
            own_far_first = step(distant, own_close[-1], 0, own_spans[0], hidden, 0)
            if layer > 0:
                index, _ = lax.optimization_barrier((index, own_far_first))
                stream = stream[index]
            last = own_far_first if layer == 0 else stream
            own_close, columns = own_close[1:], list(range(CUTS[1]))

            peer_close = [step(close, last, 0, peer_spans[0], peer_hidden)]
            peer_close.append(step(close, peer_close[0], 1, peer_spans[1], peer_hidden))
            peer_far = step(distant, peer_close[1], 0, peer_spans[0], peer_hidden, 0)
            peer_out = step(outer, peer_far, 0, peer_spans[0], [peer_close[0], peer_far], [0])
            back_first = [send_back(peer_out)]
            own_out_first = step(outer, peer_out, 0, own_spans[0], [own_close[0], own_far_first], [0])
            peer_far_second = [step(distant, own_out_first, 1, peer_spans[1], peer_hidden, 0)]
            peer_far_second.append(step(distant, peer_far_second[0], 1, peer_spans[1], peer_hidden, 1))
            last, back_second, own_far = peer_far_second[1], [], []
            for c in columns:
                if c == len(columns) // 2:
                    last = step(distant, last, 1, own_spans[1], hidden, 0)
                    own_far.append(last)
                last = step(outer, last, 1, peer_spans[1], [peer_close[1]] + peer_far_second, [c])
                back_second.append(send_back(last))
            own_far.append(step(distant, last, 1, own_spans[1], hidden, 1))
            own_out_second = step(outer, own_far[1], 1, own_spans[1], [own_close[1]] + own_far, columns)
            parts = [[own_out_first], [own_out_second], back_first, back_second]
            mixed = mix(ranges.reshape(-1), stream, gates, parts, norm_w[layer + 1] if layer + 1 < layers else None)
            stream, hidden = mixed if layer + 1 < layers else (mixed[0], None)
        return stream[orders[layers - 1][0]]

    return jax.shard_map(device_step, mesh=mesh,
                         in_specs=(token_spec, P(), P(), expert_in_spec, expert_in_spec, expert_out_spec, route_spec),
                         out_specs=token_spec, check_vma=False)
```
